32 devices in a mesh: section: 2 (over core), tensor: 2 (over x), dp: 8 (over z, y).
Axes of the slice: x: 2, y: 2, z: 4, core: 2. Of those that a mesh axis runs over, the one named last changes fastest.
Arguments:
- layer_input: bfloat16 [16, 1024, 1280], P('dp'), may hold values from -6 to 6
- out_cotangent: bfloat16 [16, 1024, 1280], P('dp'), may hold values from -6 to 6
- block_ids: int32 [16, 1024], P('dp'), may hold values from 0 to 7, never falling along the last dimension, each value on 1 to 256 neighbouring positions
- seq_lengths: int32 [16], P('dp'), may hold values from 512 to 1024, as said below
- attention_gain: bfloat16 [2, 1280], P('section', 'dp'), may hold values from 0.25 to 1.75
- query_weight: bfloat16 [2, 1280, 1280], P('section', 'dp', 'tensor'), may hold values from -0.15625 to 0.15625
- key_weight: bfloat16 [2, 1280, 320], P('section', 'dp'), may hold values from -0.15625 to 0.15625
- value_weight: bfloat16 [2, 1280, 320], P('section', 'dp'), may hold values from -0.15625 to 0.15625
- output_weight: bfloat16 [2, 1280, 1280], P('section', 'tensor', 'dp'), may hold values from -2.5 to 2.5
- swiglu_gain: bfloat16 [2, 1280], P('section', 'dp'), may hold values from 0.25 to 1.75
- gate_weight: bfloat16 [2, 1280, 3584], P('section', 'dp', 'tensor'), may hold values from -0.15625 to 0.15625
- up_weight: bfloat16 [2, 1280, 3584], P('section', 'dp', 'tensor'), may hold values from -0.15625 to 0.15625
- down_weight: bfloat16 [2, 3584, 1280], P('section', 'tensor', 'dp'), may hold values from -0.125 to 0.125
Outputs:
- activations: bfloat16 [2, 16, 1024, 1280], P('section', 'dp')
- input_grads: float32 [2, 16, 1024, 1280], P('section', 'dp')
- attention_gain_grad: float32 [2, 1280], P('section', 'dp')
- query_matrix_gradient: float32 [2, 1280, 1280], P('section', 'dp', 'tensor')
- key_weight_grad: float32 [2, 1280, 320], P('section', 'dp')
- value_weight_grad: float32 [2, 1280, 320], P('section', 'dp')
- output_weight_grad: float32 [2, 1280, 1280], P('section', 'tensor', 'dp')
- swiglu_gain_grad: float32 [2, 1280], P('section', 'dp')
- gate_weight_grad: float32 [2, 1280, 3584], P('section', 'dp', 'tensor')
- up_weight_grad: float32 [2, 1280, 3584], P('section', 'dp', 'tensor')
- down_weight_grad: float32 [2, 3584, 1280], P('section', 'tensor', 'dp')
The draws below stay inside these ranges and needn't reach their ends.
Inputs may be any that keep to these rules, and one draw needn't show every extreme that they name: `block_ids`: block numbers never fall along a sequence; a block holds 1 to 256 positions. `seq_lengths`: both ends of the range occur in every draw.
All inputs are finite; a program needn't handle non-finite values.
Results may differ from the reference program's by a relative error of at most 0.03.
Values may be sent and summed in bfloat16 or wider, within the bound.
A program may use at most 384 MiB of HBM per device.

```python
import math
import jax
import jax.numpy as jnp
import numpy as np
from jax import lax

D = 1280
HQ = 20
KVH = 5
HD = 64
FF = 3584
LEN = 1024
BLK = 256
SEQS = 16
N_SECTION = 2


def draw_seq_lengths(key, part):
    key_values, key_full, key_short = jax.random.split(key, 3)
    values = jax.random.randint(key_values, (SEQS,), LEN // 2, LEN + 1)
    where_full = jax.random.randint(key_full, (), 0, SEQS)
    where_short = (where_full + 1 + jax.random.randint(key_short, (), 0, SEQS - 1)) % SEQS
    positions = jnp.arange(SEQS)
    values = jnp.where(positions == where_full, LEN, values)
    values = jnp.where(positions == where_short, LEN // 2, values)
    return values.astype(jnp.int32)


def with_spikes(entries, stream_key, source, target, blocks, factor):
    owner, partner = [(jnp.arange(entries.shape[dim]) // (entries.shape[dim] // blocks)).reshape([-1 if axis == dim else 1 for axis in range(entries.ndim)]) for dim in (source, target)]
    chosen = jax.random.permutation(stream_key, blocks)[partner]
    strong = (owner == chosen) | (owner == (partner + blocks // 2) % blocks)
    return jnp.where(strong, factor * entries, entries)


def block_scale(own_key, shape, cuts, smallest, largest):
    def one(axis_at, blocks):
        steps = jax.random.uniform(jax.random.fold_in(jax.random.fold_in(own_key, 6), axis_at), (blocks,), jnp.float32, smallest / len(cuts), largest / len(cuts))
        return jnp.repeat(jnp.exp(steps), shape[axis_at] // blocks).reshape((-1,) + (1,) * (len(shape) - axis_at - 1))

    level = one(*cuts[0])
    for cut in cuts[1:]:
        level = level * one(*cut)
    return level


def profile(amount, total, most, skew):
    portions = [(1 << 20) // math.isqrt(standing ** skew) + 1 for standing in range(2, amount + 1)]
    surplus, counts = total - most - (amount - 1), [1] * (amount - 1)
    while surplus > 0:
        candidates = [i for i in range(amount - 1) if counts[i] < most]
        mass, left = sum([portions[i] for i in candidates]), surplus
        for i in candidates:
            extra = min(most - counts[i], max(1, left * portions[i] // mass), surplus)
            counts[i] = counts[i] + extra
            surplus = surplus - extra
    return np.array([most] + counts)


def ragged(key, amount, total, most, skew):
    if amount == 2:
        one = jax.random.randint(key, (), max(1, total - most), min(most, total - 1) + 1)
        return jnp.stack([one, total - one])
    sizes = jnp.asarray(profile(amount, total, most, skew), jnp.int32)
    couples = (amount - 1) // 2
    donor, sink = sizes[1:1 + 2 * couples:2], sizes[2:2 + 2 * couples:2]
    margin = jnp.minimum(donor - 1, most - sink)
    passed = jax.random.randint(jax.random.fold_in(key, 1), (couples,), 0, 1 << 20) % (margin + 1)
    sizes = sizes.at[1:1 + 2 * couples:2].set(donor - passed).at[2:2 + 2 * couples:2].set(sink + passed)
    return sizes[jax.random.permutation(jax.random.fold_in(key, 2), amount)]


def bell_draw(own_key, dims, deviation, most, pieces=(), kind=jnp.bfloat16):
    values = deviation * jax.random.normal(own_key, dims, jnp.float32)
    if pieces:
        values = values * block_scale(own_key, dims, pieces, -0.22, 0.18)
    return jnp.clip(values, -most, most).astype(kind)


def heavy_noise(key, shape, scale, limit, pieces, heavy, kind=jnp.bfloat16):
    drawn = scale * jax.random.normal(key, shape, jnp.float32)
    if pieces:
        drawn = drawn * block_scale(key, shape, pieces, -0.22, 0.18)
    return jnp.clip(with_spikes(drawn, jax.random.fold_in(key, 3), *heavy), -limit, limit).astype(kind)


def setup_inputs(seed: int = 0) -> dict:
    seeds = jax.random.split(jax.random.key(seed), 14)
    layer_input = heavy_noise(seeds[0], (SEQS, LEN, D), 1.0, 6.0, ((0, 8),), (0, 2, 8, 2.0))
    out_cotangent = heavy_noise(seeds[1], (SEQS, LEN, D), 1.0, 6.0, ((0, 8),), (0, 2, 8, 2.0))
    block_ids = jax.vmap(lambda own: jnp.searchsorted(jnp.cumsum(ragged(own, 2 * LEN // BLK, LEN, BLK, 0)), jnp.arange(LEN), side="right"))(jax.random.split(seeds[2], SEQS)).reshape((SEQS, LEN)).astype(jnp.int32)
    seq_lengths = draw_seq_lengths(jax.random.fold_in(seeds[13], 71), 0)
    attention_gain = jnp.clip(1.0 + 0.15 * jax.random.normal(seeds[4], (N_SECTION, D), jnp.float32), 0.25, 1.75).astype(jnp.bfloat16)
    query_weight = bell_draw(seeds[5], (N_SECTION, D, HQ * HD), D ** -0.5, 0.15625, ((0, 2), (1, 8), (2, 2)))
    key_weight = bell_draw(seeds[6], (N_SECTION, D, KVH * HD), D ** -0.5, 0.15625, ((0, 2), (1, 8)))
    value_weight = bell_draw(seeds[7], (N_SECTION, D, KVH * HD), D ** -0.5, 0.15625, ((0, 2), (1, 8)))
    output_weight = bell_draw(seeds[8], (N_SECTION, HQ * HD, D), (max(1, HQ * HD // 256)) ** -0.5, 2.5, ((0, 2), (1, 2), (2, 8)))
    swiglu_gain = jnp.clip(1.0 + 0.15 * jax.random.normal(seeds[9], (N_SECTION, D), jnp.float32), 0.25, 1.75).astype(jnp.bfloat16)
    gate_weight = bell_draw(seeds[10], (N_SECTION, D, FF), D ** -0.5, 0.15625, ((0, 2), (1, 8), (2, 2)))
    up_weight = bell_draw(seeds[11], (N_SECTION, D, FF), D ** -0.5, 0.15625, ((0, 2), (1, 8), (2, 2)))
    down_weight = bell_draw(seeds[12], (N_SECTION, FF, D), (FF // 2) ** -0.5, 0.125, ((0, 2), (1, 2), (2, 8)))
    return {"layer_input": layer_input, "out_cotangent": out_cotangent, "block_ids": block_ids, "seq_lengths": seq_lengths, "attention_gain": attention_gain, "query_weight": query_weight, "key_weight": key_weight, "value_weight": value_weight, "output_weight": output_weight, "swiglu_gain": swiglu_gain, "gate_weight": gate_weight, "up_weight": up_weight, "down_weight": down_weight}


EPSILON = 1e-05
ROPE_BASE = 10000.0
MASKED = -1e+30
TOP_PRECISION = lax.Precision.HIGHEST

@jax.custom_vjp
def low(v):
    return lax.optimization_barrier(v.astype(jnp.bfloat16)).astype(jnp.float32)

@jax.custom_vjp
def low_back(v):
    return v

def low_keep(v):
    return (low(v), None)

def low_pass(kept, grad):
    return (grad,)

def back_keep(v):
    return (v, None)

def back_low(kept, grad):
    return (low(grad),)
low.defvjp(low_keep, low_pass)
low_back.defvjp(back_keep, back_low)

def rms_scale(matrix_row_list, gain_row):
    return matrix_row_list * lax.rsqrt(lax.optimization_barrier(jnp.mean(matrix_row_list * matrix_row_list, axis=-1, keepdims=True)) + EPSILON) * gain_row

def rope_tables(length, head_size):
    positions = jnp.arange(length, dtype=jnp.float32)
    frequency = ROPE_BASE ** (-jnp.arange(head_size // 2, dtype=jnp.float32) * 2.0 / head_size)
    angles = positions[:, None] * frequency[None, :]
    return (jnp.cos(angles), jnp.sin(angles))

def rotate(values, cosine_table, sine_table):
    half_size = values.shape[-1] // 2
    lower_part = values[..., :half_size]
    upper_part = values[..., half_size:]
    cosine_wide = cosine_table[:, None, :]
    sine_wide = sine_table[:, None, :]
    return jnp.concatenate([lower_part * cosine_wide - upper_part * sine_wide, upper_part * cosine_wide + lower_part * sine_wide], axis=-1)

def project(matrix_row_list, weight_matrix):
    return jnp.einsum('pbx,xc->pbc', matrix_row_list, weight_matrix, precision=TOP_PRECISION)

def decoder_layer(section_in, params, block_rows, length_rows):
    attention_gain, query_weight, key_weight, value_weight, output_weight, swiglu_gain, gate_weight, up_weight, down_weight = params
    seq_count = section_in.shape[0]
    cosine_table, sine_table = rope_tables(LEN, HD)
    normed = low(rms_scale(section_in, attention_gain))
    queries = low(rotate(low_back(project(normed, query_weight).reshape(seq_count, LEN, HQ, HD)), cosine_table, sine_table))
    keys_all = low(rotate(low_back(project(normed, key_weight).reshape(seq_count, LEN, KVH, HD)), cosine_table, sine_table))
    values_all = low(low_back(project(normed, value_weight).reshape(seq_count, LEN, KVH, HD)))
    keys_wide = jnp.repeat(keys_all, HQ // KVH, axis=2)
    values_wide = jnp.repeat(values_all, HQ // KVH, axis=2)
    positions = jnp.arange(LEN)
    allowed = (block_rows[:, None, :] <= block_rows[:, :, None]) & (positions[None, None, :] < length_rows[:, None, None])
    score_scale = HD ** (-0.5)

    def one_head(head_parts):
        query_head, key_head, value_head = head_parts
        scores = low_back(jnp.einsum('sqd,skd->sqk', query_head, key_head, precision=TOP_PRECISION)) * score_scale
        softmax_rows = low(jax.nn.softmax(jnp.where(allowed, scores, MASKED), axis=-1))
        return jnp.einsum('sqk,skd->sqd', softmax_rows, value_head, precision=TOP_PRECISION)
    mixed_heads = lax.map(jax.checkpoint(one_head), (queries.transpose(2, 0, 1, 3), keys_wide.transpose(2, 0, 1, 3), values_wide.transpose(2, 0, 1, 3)))
    mixed_rows = low(low_back(mixed_heads.transpose(1, 2, 0, 3).reshape(seq_count, LEN, HQ * HD)))
    middle = section_in + low_back(project(mixed_rows, output_weight))
    normed_second = low(rms_scale(middle, swiglu_gain))
    gate_rows = low_back(project(normed_second, gate_weight))
    up_rows = low_back(project(normed_second, up_weight))
    hidden = low(jax.nn.silu(gate_rows) * up_rows)
    return middle + low_back(project(hidden, down_weight))

def reference(layer_input, out_cotangent, block_ids, seq_lengths, attention_gain, query_weight, key_weight, value_weight, output_weight, swiglu_gain, gate_weight, up_weight, down_weight):
    weights = (attention_gain, query_weight, key_weight, value_weight, output_weight, swiglu_gain, gate_weight, up_weight, down_weight)
    params_early = tuple((weight_matrix[0].astype(jnp.float32) for weight_matrix in weights))
    params_late = tuple((weight_matrix[1].astype(jnp.float32) for weight_matrix in weights))
    group_size = math.gcd(SEQS, max(1, 4096 // LEN))
    group_count = SEQS // group_size
    inputs_grouped = layer_input.astype(jnp.float32).reshape(group_count, group_size, LEN, D)
    cotangents_grouped = out_cotangent.astype(jnp.float32).reshape(group_count, group_size, LEN, D)
    blocks_grouped = block_ids.reshape(group_count, group_size, LEN)
    lengths_grouped = seq_lengths.reshape(group_count, group_size)

    def scan_step(totals, item_parts):
        section_in, cotangent, block_rows, length_rows = item_parts

        def run_layer(matrix_row_list, params):
            return decoder_layer(matrix_row_list, params, block_rows, length_rows)
        early_out, early_back = jax.vjp(run_layer, section_in, params_early)
        middle_in = low(early_out)
        late_out, late_back = jax.vjp(run_layer, middle_in, params_late)
        middle_grad, late_grads = late_back(cotangent)
        input_grad, early_grads = early_back(middle_grad)
        early_totals = tuple((running_sum + new_sum for running_sum, new_sum in zip(totals[0], early_grads)))
        late_totals = tuple((running_sum + new_sum for running_sum, new_sum in zip(totals[1], late_grads)))
        return ((early_totals, late_totals), (middle_in.astype(jnp.bfloat16), late_out.astype(jnp.bfloat16), input_grad, middle_grad))
    zero_totals = (tuple((jnp.zeros_like(array_part) for array_part in params_early)), tuple((jnp.zeros_like(array_part) for array_part in params_late)))
    totals, outputs = lax.scan(scan_step, zero_totals, (inputs_grouped, cotangents_grouped, blocks_grouped, lengths_grouped))
    acts_early, acts_late, grads_early, grads_late = outputs
    activations = jnp.stack([acts_early.reshape(SEQS, LEN, D), acts_late.reshape(SEQS, LEN, D)])
    input_grads = jnp.stack([grads_early.reshape(SEQS, LEN, D), grads_late.reshape(SEQS, LEN, D)])
    gradients = tuple((jnp.stack([early_part, later_portion]) for early_part, later_portion in zip(totals[0], totals[1])))
    return (activations, input_grads, gradients[0], gradients[1], gradients[2], gradients[3], gradients[4], gradients[5], gradients[6], gradients[7], gradients[8])
```

```python
import jax
import jax.numpy as jnp
from jax import lax
from jax.experimental import pallas as pl
from jax.experimental.pallas import tpu as pltpu
from jax.sharding import PartitionSpec as P

HQ = 20
KVH = 5
HD = 64
PAIR = 2 * HD
EPSILON = 1e-05
ROPE_BASE = 10000.0
MASKED = -1e30
LOW = jnp.bfloat16
WIDE = jnp.float32
FLIP = ((0, 1), (1, 0))


def dot_nn(a, b):
    return lax.dot_general(a, b, (((1,), (0,)), ((), ())), preferred_element_type=WIDE)


def dot_nt(a, b):
    return lax.dot_general(a, b, (((1,), (1,)), ((), ())), preferred_element_type=WIDE)


def dot_tn(a, b):
    return lax.dot_general(a, b, (((0,), (0,)), ((), ())), preferred_element_type=WIDE)


def rope_kernel(kv_pairs, scale, x_ref, cos_ref, sin_ref, cos_kv_ref, sin_kv_ref, q_ref, kv_ref):
    rows = x_ref.shape[0]
    lane = lax.broadcasted_iota(jnp.int32, (rows, PAIR), 1)
    lower = lane % HD < HD // 2
    q_pairs = x_ref.shape[1] // PAIR - kv_pairs
    for pair in range(q_pairs + kv_pairs):
        x = x_ref[:, pair * PAIR : (pair + 1) * PAIR]
        turned = jnp.where(lower, pltpu.roll(x, PAIR - HD // 2, 1), pltpu.roll(x, HD // 2, 1))
        if pair < q_pairs:
            y = (x * cos_ref[...] + turned * sin_ref[...]) * scale
            q_ref[:, pair * PAIR : (pair + 1) * PAIR] = y.astype(LOW)
        else:
            y = x * cos_kv_ref[...] + turned * sin_kv_ref[...]
            at = (pair - q_pairs) * PAIR
            kv_ref[:, at : at + PAIR] = y.astype(LOW)


def rope_rows(qkv, tables, kv_width, scale):
    rows, width = qkv.shape
    q_width = width - kv_width
    block = min(rows, 128)
    row_spec = lambda cols: pl.BlockSpec((block, cols), lambda i: (i, 0))
    kernel = lambda *refs: rope_kernel(kv_width // PAIR, scale, *refs)
    return pl.pallas_call(
        kernel,
        grid=(rows // block,),
        in_specs=[row_spec(width)] + [row_spec(PAIR)] * 4,
        out_specs=[row_spec(q_width), row_spec(kv_width)],
        out_shape=[
            jax.ShapeDtypeStruct((rows, q_width), LOW),
            jax.ShapeDtypeStruct((rows, kv_width), LOW),
        ],
        name="rope_rows",
    )(qkv, *tables)


def unrope_kernel(dq_ref, dkv_ref, cos_ref, sin_ref, cos_kv_ref, sin_kv_ref, out_ref):
    rows = dq_ref.shape[0]
    lane = lax.broadcasted_iota(jnp.int32, (rows, PAIR), 1)
    lower = lane % HD < HD // 2
    q_pairs = dq_ref.shape[1] // PAIR
    for pair in range(out_ref.shape[1] // PAIR):
        if pair < q_pairs:
            x = dq_ref[:, pair * PAIR : (pair + 1) * PAIR].astype(WIDE)
            cos, sin = cos_ref, sin_ref
        else:
            x = dkv_ref[:, (pair - q_pairs) * PAIR : (pair - q_pairs + 1) * PAIR]
            cos, sin = cos_kv_ref, sin_kv_ref
        turned = jnp.where(lower, pltpu.roll(x, PAIR - HD // 2, 1), pltpu.roll(x, HD // 2, 1))
        out_ref[:, pair * PAIR : (pair + 1) * PAIR] = (x * cos[...] - turned * sin[...]).astype(LOW)


def unrope_rows(dq, dkv, tables):
    rows = dq.shape[0]
    width = dq.shape[1] + dkv.shape[1]
    block = min(rows, 128)
    row_spec = lambda cols: pl.BlockSpec((block, cols), lambda i: (i, 0))
    return pl.pallas_call(
        unrope_kernel,
        grid=(rows // block,),
        in_specs=[row_spec(dq.shape[1]), row_spec(dkv.shape[1])] + [row_spec(PAIR)] * 4,
        out_specs=row_spec(width),
        out_shape=jax.ShapeDtypeStruct((rows, width), LOW),
        name="unrope_rows",
    )(dq, dkv, *tables)


def attend_kernel(q_ref, kv_ref, bias_ref, out_ref, log_ref):
    half = q_ref.shape[0] // 2
    for part in range(2):
        span = kv_ref.shape[0] * (3 + part) // 4
        rows = slice(part * half, (part + 1) * half)
        for head in range(2):
            lanes = slice(head * HD, (head + 1) * HD)
            scores = dot_nt(q_ref[rows, lanes], kv_ref[:span, :HD]) + bias_ref[rows, :span]
            peak = jnp.max(scores, axis=-1, keepdims=True)
            weights = jnp.exp(scores - peak)
            total = jnp.sum(weights, axis=-1, keepdims=True)
            mixed = dot_nn(weights.astype(LOW), kv_ref[:span, HD:]) / total
            out_ref[rows, lanes] = mixed.astype(LOW)
            log_ref[rows, lanes] = jnp.broadcast_to(peak + jnp.log(total), (half, HD))


def attend(q, kv, bias):
    rows, width = q.shape
    full = kv.shape[0]
    group = width // kv.shape[1]
    pairs = width // PAIR
    q_spec = pl.BlockSpec((rows, PAIR), lambda p: (0, p))
    return pl.pallas_call(
        attend_kernel,
        grid=(pairs,),
        in_specs=[
            q_spec,
            pl.BlockSpec((full, PAIR), lambda p: (0, p // group)),
            pl.BlockSpec((rows, full), lambda p: (0, 0)),
        ],
        out_specs=[q_spec, q_spec],
        out_shape=[jax.ShapeDtypeStruct((rows, width), LOW), jax.ShapeDtypeStruct((rows, width), WIDE)],
        name="attend",
    )(q, kv, bias)


def attend_back_kernel(group, q_ref, kv_ref, bias_ref, log_ref, dout_ref, dq_ref, dkv_ref):
    half = q_ref.shape[0] // 2

    @pl.when(pl.program_id(0) % group == 0)
    def _():
        dkv_ref[...] = jnp.zeros_like(dkv_ref)

    for part in range(2):
        span = kv_ref.shape[0] * (3 + part) // 4
        rows = slice(part * half, (part + 1) * half)
        for head in range(2):
            lanes = slice(head * HD, (head + 1) * HD)
            q = q_ref[rows, lanes]
            dout = dout_ref[rows, lanes]
            keys = kv_ref[:span, :HD]
            scores = dot_nt(q, keys) + bias_ref[rows, :span]
            probs = jnp.exp(scores - log_ref[rows, head * HD : head * HD + 1])
            dprobs = dot_nt(dout, kv_ref[:span, HD:])
            both = probs * dprobs
            row_dot = jnp.sum(both, axis=-1, keepdims=True)
            dscores = (both - probs * row_dot).astype(LOW)
            dq_ref[rows, lanes] = dot_nn(dscores, keys) * HD ** (-0.5)
            dkv_ref[:span, :HD] += dot_tn(dscores, q)
            dkv_ref[:span, HD:] += dot_tn(probs.astype(LOW), dout)


def attend_back(q, kv, bias, log_total, dout):
    rows, width = q.shape
    full = kv.shape[0]
    group = width // kv.shape[1]
    pairs = width // PAIR
    q_spec = pl.BlockSpec((rows, PAIR), lambda p: (0, p))
    kv_spec = pl.BlockSpec((full, PAIR), lambda p: (0, p // group))
    kernel = lambda *refs: attend_back_kernel(group, *refs)
    return pl.pallas_call(
        kernel,
        grid=(pairs,),
        in_specs=[q_spec, kv_spec, pl.BlockSpec((rows, full), lambda p: (0, 0)), q_spec, q_spec],
        out_specs=[q_spec, kv_spec],
        out_shape=[
            jax.ShapeDtypeStruct((rows, width), WIDE),
            jax.ShapeDtypeStruct((full, kv.shape[1]), WIDE),
        ],
        name="attend_back",
    )(q, kv, bias, log_total, dout)


def flip_section(x):
    return lax.ppermute(x, "section", FLIP)


def flip_tensor(x):
    return lax.ppermute(x, "tensor", FLIP)


class Spread:
    def __init__(self, count, width):
        self.count = count
        self.width = width
        self.half = width // count // 2
        self.grid = count == 8

    def places(self):
        section = lax.axis_index("section")
        own = lax.axis_index("dp")
        place = jnp.arange(self.width)
        side = place // (self.width // 2)
        rest = place % (self.width // 2)
        inner = rest % self.half
        block = rest // self.half
        if self.grid:
            plane, back = block // 4, block % 4
            shard = ((own // 2 - back) % 4) * 2 + (own % 2 + plane) % 2
        else:
            shard = block
        return (shard * 2 + (section + side) % 2) * self.half + inner

    def shift(self, x, by):
        pairs = [(i, ((i // 2 + by) % 4) * 2 + i % 2) for i in range(8)]
        return lax.ppermute(x, "dp", pairs)

    def flip_plane(self, x):
        return lax.ppermute(x, "dp", [(i, i ^ 1) for i in range(8)])

    def gather(self, piece):
        if not self.grid:
            own = lax.all_gather(piece, "dp", axis=0, tiled=True)
            return [own, flip_section(own)]
        column = jnp.concatenate([piece] + [self.shift(piece, by) for by in (1, 2, 3)], axis=0)
        other = self.flip_plane(column)
        return [column, other, flip_section(column), flip_section(other)]

    def scatter(self, own_half):
        if not self.grid:
            return lax.psum_scatter(own_half, "dp", scatter_dimension=0, tiled=True).astype(WIDE)
        cut = self.width // 4
        received = self.flip_plane(own_half[cut:])
        column = (own_half[:cut].astype(WIDE) + received.astype(WIDE)).astype(LOW)
        size = self.half
        total = column[:size].astype(WIDE)
        for back in (1, 2, 3):
            total = total + self.shift(column[back * size : (back + 1) * size], -back).astype(WIDE)
        return total


def joined(parts, start, stop):
    return jnp.concatenate([part[:, start:stop] for part in parts], axis=0)


def grad_half(left, right):
    half = left.shape[1] // 2
    received = flip_section(dot_tn(left[:, half:], right).astype(LOW))
    return (dot_tn(left[:, :half], right) + received.astype(WIDE)).astype(LOW)


def scale_of(x):
    return lax.rsqrt(jnp.mean(x * x, axis=-1, keepdims=True) + EPSILON)


def norm_back(x, inverse, gain, dnormed):
    u = dnormed * gain
    back = u * inverse - x * (jnp.mean(u * x, axis=-1, keepdims=True) * (inverse * inverse * inverse))
    gain_grad = jnp.sum(dnormed * x * inverse, axis=0)
    return back, gain_grad


def on_device(
    layer_input,
    out_cotangent,
    block_ids,
    seq_lengths,
    attention_gain,
    query_weight,
    key_weight,
    value_weight,
    output_weight,
    swiglu_gain,
    gate_weight,
    up_weight,
    down_weight,
):
    first = lax.axis_index("section") == 0
    lead = lax.axis_index("tensor") == 0
    width = layer_input.shape[2]
    full = layer_input.shape[1]
    block = full // 4
    rows = 2 * block
    hidden_width = gate_weight.shape[2]
    q_half = query_weight.shape[2]
    q_width = 2 * q_half
    kv_width = key_weight.shape[2] * 2
    spread = Spread(lax.axis_size("dp"), width)
    half = spread.half

    def pick(a, b):
        return jnp.where(first, a, b)

    def own_blocks(x):
        quarters = [x[i * block : (i + 1) * block] for i in range(4)]
        return jnp.concatenate([pick(quarters[0], quarters[1]), pick(quarters[3], quarters[2])], axis=0)

    def all_blocks(own, other):
        return jnp.concatenate(
            [
                pick(own[:block], other[:block]),
                pick(other[:block], own[:block]),
                pick(other[block:], own[block:]),
                pick(own[block:], other[block:]),
            ],
            axis=0,
        )

    shard = width // lax.axis_size("dp")
    q_own = query_weight[0]
    o_own = output_weight[0].T
    both = jnp.concatenate([q_own, o_own], axis=1)
    both_other = flip_tensor(both)
    sides = (jnp.where(lead, both, both_other), jnp.where(lead, both_other, both))
    kv_own = jnp.stack(
        [key_weight[0].reshape(shard, KVH, HD), value_weight[0].reshape(shard, KVH, HD)], axis=2
    ).reshape(shard, kv_width)
    gains = jnp.concatenate(
        [attention_gain[0][:, None], swiglu_gain[0][:, None], jnp.zeros((shard, PAIR - 2), LOW)], axis=1
    )
    attention_pack = jnp.concatenate(
        [sides[0][:, :q_half], sides[1][:, :q_half], kv_own, sides[0][:, q_half:], sides[1][:, q_half:], gains],
        axis=1,
    )
    swiglu_pack = jnp.concatenate([gate_weight[0], up_weight[0], down_weight[0].T], axis=1)

    def by_layer(pack):
        kept = pick(pack[:half], pack[half:])
        received = flip_section(pick(pack[half:], pack[:half]))
        return pick(kept, received), pick(received, kept)

    attention_pieces = by_layer(attention_pack)
    swiglu_pieces = by_layer(swiglu_pack)
    weights = []
    for layer in range(2):
        parts = spread.gather(attention_pieces[layer])
        o_start = q_width + kv_width
        qkv_weight = joined(parts, 0, o_start)
        out_weight = joined(parts, o_start, o_start + q_width)
        gain_rows = joined(parts, o_start + q_width, o_start + q_width + PAIR)[:, :2].T.astype(WIDE)
        parts = spread.gather(swiglu_pieces[layer])
        gate_up = joined(parts, 0, 2 * hidden_width)
        down = joined(parts, 2 * hidden_width, 3 * hidden_width)
        weights.append((qkv_weight, out_weight, gain_rows[0:1], gain_rows[1:2], gate_up, down))

    tensor_at = lax.axis_index("tensor")
    places = spread.places()
    order = (jnp.arange(width)[:, None] == places[None, :]).astype(LOW)
    x = dot_nn(own_blocks(lax.dynamic_index_in_dim(layer_input, tensor_at, 0, False)), order)
    cotangent = dot_nn(
        own_blocks(lax.dynamic_index_in_dim(out_cotangent, tensor_at, 0, False)), order
    )

    block_row = lax.dynamic_index_in_dim(block_ids, tensor_at, 0, False)
    length = lax.dynamic_index_in_dim(seq_lengths, tensor_at, 0, False)
    key_at = jnp.arange(full)
    own_ids = own_blocks(block_row)
    allowed = (block_row[None, :] <= own_ids[:, None]) & (key_at < length)[None, :]
    bias = jnp.where(allowed, 0.0, MASKED).astype(WIDE)

    row_at = own_blocks(key_at).astype(WIDE)[:, None]
    lane = jnp.arange(PAIR)
    frequency = ROPE_BASE ** (-(lane % (HD // 2)).astype(WIDE) * 2.0 / HD)
    angle = row_at * frequency[None, :]
    cosine, sine = jnp.cos(angle), jnp.sin(angle)
    sine = jnp.where((lane % HD < HD // 2)[None, :], -sine, sine)
    is_key = (lane < HD)[None, :]
    tables = (cosine, sine, jnp.where(is_key, cosine, 1.0), jnp.where(is_key, sine, 0.0))

    saved = []
    outputs = []
    for layer in range(2):
        qkv_weight, out_weight, gain, second_gain, gate_up, down = weights[layer]
        inverse = scale_of(x)
        normed = (x * inverse * gain).astype(LOW)
        q, kv_rows = rope_rows(dot_nn(normed, qkv_weight), tables, kv_width, HD ** (-0.5))
        kv = all_blocks(kv_rows, flip_section(kv_rows))
        mixed, log_total = attend(q, kv, bias)
        middle = x + dot_nt(mixed, out_weight)
        second_inverse = scale_of(middle)
        second = (middle * second_inverse * second_gain).astype(LOW)
        second_all = jnp.concatenate([second, flip_tensor(second)], axis=0)
        gate_rows = dot_nn(second_all, gate_up).astype(LOW)
        gate = gate_rows[:, :hidden_width].astype(WIDE)
        up = gate_rows[:, hidden_width:].astype(WIDE)
        hidden = (gate * jax.nn.sigmoid(gate) * up).astype(LOW)
        away = flip_tensor(dot_nt(hidden[rows:], down).astype(LOW))
        y = middle + (dot_nt(hidden[:rows], down) + away.astype(WIDE))
        saved.append((x, inverse, normed, q, kv, mixed, log_total, middle, second_inverse, second_all, gate_rows, hidden))
        low = y.astype(LOW)
        outputs.append(low)
        x = low.astype(WIDE)

    dy = cotangent
    grads = [None, None]
    input_grads = [None, None]
    for layer in (1, 0):
        qkv_weight, out_weight, gain, second_gain, gate_up, down = weights[layer]
        x, inverse, normed, q, kv, mixed, log_total, middle, second_inverse, second_all, gate_rows, hidden = saved[layer]
        dy_low = dy.astype(LOW)
        dy_all = jnp.concatenate([dy_low, flip_tensor(dy_low)], axis=0)
        dhidden = dot_nn(dy_all, down).astype(LOW).astype(WIDE)
        gate = gate_rows[:, :hidden_width].astype(WIDE)
        up = gate_rows[:, hidden_width:].astype(WIDE)
        sig = jax.nn.sigmoid(gate)
        dgate_up = jnp.concatenate(
            [
                (dhidden * up * sig * (1.0 + gate * (1.0 - sig))).astype(LOW),
                (dhidden * gate * sig).astype(LOW),
            ],
            axis=1,
        )
        away = flip_tensor(dot_nt(dgate_up[rows:], gate_up).astype(LOW))
        dsecond = dot_nt(dgate_up[:rows], gate_up) + away.astype(WIDE)
        swiglu_half = jnp.concatenate([grad_half(second_all, dgate_up), grad_half(dy_all, hidden)], axis=1)
        swiglu_grad = spread.scatter(swiglu_half)
        back, second_gain_grad = norm_back(middle, second_inverse, second_gain, dsecond)
        dmiddle = dy + back
        dmiddle_low = dmiddle.astype(LOW)
        out_grad = spread.scatter(grad_half(dmiddle_low, mixed))
        dmixed = dot_nn(dmiddle_low, out_weight).astype(LOW)
        dq, dkv_all = attend_back(q, kv, bias, log_total, dmixed)
        quarters = [dkv_all[i * block : (i + 1) * block] for i in range(4)]
        sent = jnp.concatenate([pick(quarters[1], quarters[0]), pick(quarters[2], quarters[3])], axis=0)
        dkv = own_blocks(dkv_all) + flip_section(sent)
        dqkv = unrope_rows(dq, dkv, tables)
        dnormed = dot_nt(dqkv, qkv_weight)
        back, gain_grad = norm_back(x, inverse, gain, dnormed)
        dx = dmiddle + back
        gain_pair = jnp.concatenate(
            [gain_grad[:, None], second_gain_grad[:, None], jnp.zeros((width, PAIR - 2), WIDE)], axis=1
        )
        gain_half = (
            gain_pair[: width // 2] + flip_section(gain_pair[width // 2 :].astype(LOW)).astype(WIDE)
        ).astype(LOW)
        qkv_grad = spread.scatter(jnp.concatenate([grad_half(normed, dqkv), gain_half], axis=1))
        q_keep = jnp.where(lead, qkv_grad[:, :q_half], qkv_grad[:, q_half:q_width])
        q_send = jnp.where(lead, qkv_grad[:, q_half:q_width], qkv_grad[:, :q_half])
        o_keep = jnp.where(lead, out_grad[:, :q_half], out_grad[:, q_half:])
        o_send = jnp.where(lead, out_grad[:, q_half:], out_grad[:, :q_half])
        rest = qkv_grad[:, q_width:]
        received = flip_tensor(jnp.concatenate([q_send, o_send, rest], axis=1).astype(LOW)).astype(WIDE)
        kept = jnp.concatenate([q_keep, o_keep, rest], axis=1) + received
        grads[layer] = jnp.concatenate([kept, swiglu_grad], axis=1)
        input_grads[layer] = dx.astype(LOW)
        dy = dx

    sent = flip_section(pick(grads[1], grads[0]))
    mine = pick(grads[0], grads[1])
    total = jnp.concatenate([pick(mine, sent), pick(sent, mine)], axis=0)

    def spread_rows(pair):
        sets = []
        for part in pair:
            plain = dot_nt(part, order).astype(LOW)
            sets.append(jnp.stack([plain, flip_tensor(plain)], axis=0))
        received = flip_section(pick(sets[1], sets[0]))
        own = pick(sets[0], sets[1])
        near = all_blocks(own[0], received[0])
        far = all_blocks(own[1], received[1])
        return jnp.stack([jnp.where(lead, near, far), jnp.where(lead, far, near)], axis=0)

    activations = spread_rows(outputs)
    all_grads = spread_rows(input_grads).astype(WIDE)
    kv_start = 2 * q_half
    kv_grad = total[:, kv_start : kv_start + kv_width].reshape(shard, KVH, 2, HD)
    gain_start = kv_start + kv_width
    ffn = gain_start + PAIR
    return (
        activations[None],
        all_grads[None],
        total[:, gain_start][None],
        total[:, :q_half][None],
        kv_grad[:, :, 0].reshape(shard, KVH * HD)[None],
        kv_grad[:, :, 1].reshape(shard, KVH * HD)[None],
        total[:, q_half : 2 * q_half].T[None],
        total[:, gain_start + 1][None],
        total[:, ffn : ffn + hidden_width][None],
        total[:, ffn + hidden_width : ffn + 2 * hidden_width][None],
        total[:, ffn + 2 * hidden_width :].T[None],
    )


def solution(mesh):
    return jax.shard_map(
        on_device,
        mesh=mesh,
        in_specs=(
            P("dp", None, None),
            P("dp", None, None),
            P("dp", None),
            P("dp"),
            P("section", "dp"),
            P("section", "dp", "tensor"),
            P("section", "dp", None),
            P("section", "dp", None),
            P("section", "tensor", "dp"),
            P("section", "dp"),
            P("section", "dp", "tensor"),
            P("section", "dp", "tensor"),
            P("section", "tensor", "dp"),
        ),
        out_specs=(
            P("section", "dp", None, None),
            P("section", "dp", None, None),
            P("section", "dp"),
            P("section", "dp", "tensor"),
            P("section", "dp", None),
            P("section", "dp", None),
            P("section", "tensor", "dp"),
            P("section", "dp"),
            P("section", "dp", "tensor"),
            P("section", "dp", "tensor"),
            P("section", "tensor", "dp"),
        ),
        check_vma=False,
    )
```
